32 devices in a mesh: gx: 4 (over z), gy: 8 (over y, x, core).
Axes of the slice: x: 2, y: 2, z: 4, core: 2. Of those that a mesh axis runs over, the one named last changes fastest.
Arguments:
- spectrum: float32 [2, 256, 16384], P(None, ('gx', 'gy')), may hold values from -6 to 6
- parameters: float32 [2], replicated, may hold values from -1.5 to 1.5
Outputs:
- advanced: float32 [2, 256, 16384], P(None, ('gx', 'gy'))
The draws below stay inside these ranges and needn't reach their ends.
All inputs are finite; a program needn't handle non-finite values.
Results may differ from the reference program's by a relative error of at most 0.0003.
Values sent between devices are 32-bit elements; how exact they have to be, the bound alone decides.
A program may use at most 128 MiB of HBM per device.

```python
import math
import jax
import jax.numpy as jnp

COLS = 16384
STEPS = 1
ROWS = 256


def levels(own_key, shape, pieces, least, largest):
    factor_of, own = 1.0, jax.random.fold_in(own_key, 6)
    for dim, parts in pieces:
        draws = jnp.exp(jax.random.uniform(jax.random.fold_in(own, dim), (parts,), jnp.float32, least / len(pieces), largest / len(pieces)))
        factor_of = factor_of * jnp.repeat(draws, shape[dim] // parts).reshape([-1 if axis == dim else 1 for axis in range(len(shape))])
    return factor_of


def scatter_about(own_key, extent, deviation, limit, pieces=(), held_as=jnp.bfloat16):
    factor_of = levels(own_key, extent, pieces, -0.22, 0.18) if pieces else 1.0
    array = jax.random.normal(own_key, extent, jnp.float32) * deviation * factor_of
    return jnp.minimum(jnp.maximum(array, -limit), limit).astype(held_as)


def setup_inputs(seed: int = 0) -> dict:
    seeds = jax.random.split(jax.random.key(seed), 3)
    return {
        "spectrum": scatter_about(seeds[0], (2, ROWS, COLS), 1.0, 6.0, ((1, 32),), jnp.float32),
        "parameters": jnp.clip(jax.random.uniform(seeds[1], (2,), jnp.float32, -1.5, 1.5), -1.5, 1.5),
    }


time_step = 0.1
spacing = 0.25


def phi_series(zeta):
    result = []
    for phi_order in (1, 2, 3):
        running = jnp.full_like(zeta, 1.0 / math.factorial(14 + phi_order))
        for degree in range(13, -1, -1):
            running = running * zeta + 1.0 / math.factorial(degree + phi_order)
        result.append(running)
    return result


def phi_values(zeta):
    inside = zeta.real * zeta.real + zeta.imag * zeta.imag < 1.0
    guarded = jnp.where(inside, jnp.ones_like(zeta), zeta)
    series = phi_series(zeta)
    phi_one = (jnp.exp(guarded) - 1.0) / guarded
    phi_two = (phi_one - 1.0) / guarded
    phi_three = (phi_two - 0.5) / guarded
    direct = [phi_one, phi_two, phi_three]
    return [jnp.where(inside, series[index], direct[index]) for index in range(3)]


def reference(spectrum, parameters):
    rows_all = spectrum.shape[1]
    columns = spectrum.shape[2]
    modes_total = rows_all * columns
    current = (spectrum[0] + 1j * spectrum[1]).reshape(modes_total)
    mode_index = jnp.arange(modes_total, dtype=jnp.int32)
    signed = jnp.where(mode_index < modes_total // 2, mode_index, mode_index - modes_total).astype(spectrum.dtype)
    wavenum = signed * (2.0 * math.pi / (modes_total * spacing))
    wave_square = wavenum * wavenum
    dispersion = parameters[0]
    cubic_twist = parameters[1]
    zeta = time_step * (1.0 - wave_square) - 1j * (time_step * dispersion * wave_square)
    phi_one, phi_two, phi_three = phi_values(zeta)
    half_weight = 0.5 * time_step * phi_values(zeta / 2.0)[0]
    decay_full = jnp.exp(zeta)
    decay_half = jnp.exp(zeta / 2.0)
    weight_one = time_step * (phi_one - 3.0 * phi_two + 4.0 * phi_three)
    weight_two = time_step * (phi_two - 2.0 * phi_three)
    weight_three = time_step * (4.0 * phi_three - phi_two)

    def nonlinear(spectral):
        physical = jnp.fft.ifft(spectral, norm="ortho")
        magnitude = physical.real * physical.real + physical.imag * physical.imag
        cubic = -(1.0 + 1j * cubic_twist) * magnitude * physical
        return jnp.fft.fft(cubic, norm="ortho")

    for repeat in range(STEPS):
        start_term = nonlinear(current)
        inner_one = decay_half * current + half_weight * start_term
        one_term = nonlinear(inner_one)
        inner_two = decay_half * current + half_weight * one_term
        two_term = nonlinear(inner_two)
        inner_three = decay_half * inner_one + half_weight * (2.0 * two_term - start_term)
        three_term = nonlinear(inner_three)
        current = (decay_full * current + weight_one * start_term
                   + 2.0 * weight_two * (one_term + two_term) + weight_three * three_term)
    return jnp.stack([current.real, current.imag]).reshape(2, rows_all, columns)
```

```python
import functools
import math

import jax
import jax.numpy as jnp
import numpy as np
from jax import lax
from jax.experimental import pallas as pl
from jax.experimental.pallas import tpu as pltpu
from jax.sharding import PartitionSpec as P

time_step = 0.1
spacing = 0.25
lanes = 128
sublanes = 8


def real_form(matrix):
    return np.block([[matrix.real, -matrix.imag], [matrix.imag, matrix.real]])


def halves(matrix):
    high = jnp.asarray(matrix, jnp.float32).astype(jnp.bfloat16)
    low = (jnp.asarray(matrix, jnp.float32) - high.astype(jnp.float32)).astype(jnp.bfloat16)
    return high, low


def unit_roots(left, right, length):
    product = (left[:, None].astype(np.int64) * right[None, :].astype(np.int64)) % length
    return np.exp(2j * np.pi * product / length)


def split(value):
    high = value.astype(jnp.bfloat16)
    return high, (value - high.astype(jnp.float32)).astype(jnp.bfloat16)


def dot(a, b):
    return jnp.dot(a, b, preferred_element_type=jnp.float32)


def dot3(left, right):
    return dot(left[0], right[0]) + dot(left[0], right[1]) + dot(left[1], right[0])


def times(a, b):
    return a[0] * b[0] - a[1] * b[1], a[0] * b[1] + a[1] * b[0]


def phi_values(w, orders):
    inside = w[0] * w[0] + w[1] * w[1] < 1.0
    g = (jnp.where(inside, 1.0, w[0]), jnp.where(inside, 0.0, w[1]))
    inverse = 1.0 / (g[0] * g[0] + g[1] * g[1])
    inv = (g[0] * inverse, -g[1] * inverse)
    growth = jnp.exp(g[0])
    direct = []
    last = (growth * jnp.cos(g[1]), growth * jnp.sin(g[1]))
    for k in range(orders):
        last = times((last[0] - 1.0 / math.factorial(k), last[1]), inv)
        direct.append(last)
    running = (
        jnp.full_like(w[0], 1.0 / math.factorial(14 + orders)),
        jnp.zeros_like(w[0]),
    )
    for degree in range(13, -1, -1):
        running = times(running, w)
        running = (running[0] + 1.0 / math.factorial(degree + orders), running[1])
    series = [running]
    for k in range(orders - 1, 0, -1):
        running = times(running, w)
        running = (running[0] + 1.0 / math.factorial(k), running[1])
        series.insert(0, running)
    return [
        (jnp.where(inside, s[0], d[0]), jnp.where(inside, s[1], d[1]))
        for s, d in zip(series, direct)
    ]


def weights_at(mode, modes_total, dispersion):
    signed = jnp.where(mode < modes_total // 2, mode, mode - modes_total).astype(jnp.float32)
    wavenum = signed * (2.0 * math.pi / (modes_total * spacing))
    square = wavenum * wavenum
    zeta = (time_step * (1.0 - square), -(time_step * dispersion * square))
    half = (0.5 * zeta[0], 0.5 * zeta[1])
    one, two, three = phi_values(zeta, 3)
    (half_one,) = phi_values(half, 1)
    grow = jnp.exp(half[0])
    e2 = (grow * jnp.cos(half[1]), grow * jnp.sin(half[1]))
    full = times(e2, e2)
    h = time_step
    q = tuple(0.5 * h * x for x in half_one)
    f1 = tuple(h * (a - 3.0 * b + 4.0 * c) for a, b, c in zip(one, two, three))
    f2 = tuple(2.0 * h * (b - 2.0 * c) for b, c in zip(two, three))
    f3 = tuple(h * (4.0 * c - b) for b, c in zip(two, three))
    return full, e2, q, f1, f2, f3


def kernel(
    axes, sizes,
    par_ref, spec_ref, m1h, m1l, m2h, m2l, n2h, n2l, m3h, m3l, n3h, n3l, t2_ref,
    out_ref,
    send, recv, wts, t1, pre, acc, astate, nl, xah, xal, xbh, xbl, pxh, pxl, send_sem, recv_sem,
):
    Z, G, D, K, R = sizes
    A = K * D
    cols = A * lanes
    span = K * lanes
    total = R * cols
    zi = lax.axis_index(axes[0])
    gi = lax.axis_index(axes[1])
    me = zi * G + gi
    mesh_type = pl.DeviceIdType.MESH
    beta = par_ref[1]

    chunks = 2 if K % 2 == 0 else 1
    part_k = K // chunks

    def peer_at(i):
        mask = D - i
        if D & (D - 1) == 0:
            peer, bit = 0, 1
            while bit < D:
                peer = peer + lax.rem(me // bit + mask // bit, 2) * bit
                bit *= 2
        else:
            peer = lax.rem(me + mask, D)
        return peer // G, lax.rem(peer, G)

    def copy(slot, chunk, i, landing):
        pz, pg = peer_at(i)
        peer = pz * G + pg
        at = me if landing is None else peer
        ks = pl.ds(chunk * part_k, part_k)
        return pltpu.make_async_remote_copy(
            src_ref=send.at[:, ks, peer],
            dst_ref=recv.at[slot, :, ks, at],
            send_sem=send_sem.at[chunk, peer],
            recv_sem=recv_sem.at[slot, chunk, at],
            device_id=(pz, pg),
            device_id_type=mesh_type,
        )

    def start(slot, chunk):
        def body(i, carry):
            copy(slot, chunk, i, None).start()
            return carry

        lax.fori_loop(1, D, body, 0)
        for k in range(chunk * part_k, (chunk + 1) * part_k):
            recv[slot, :, k, me] = send[:, k, me]

    def finish(slot, chunk):
        def body(i, carry):
            arriving = copy(slot, chunk, i, True)
            arriving.wait_recv()
            arriving.wait_send()
            return carry

        lax.fori_loop(1, D, body, 0)

    def loop(count, body):
        def wrapped(i, carry):
            body(i)
            return carry

        lax.fori_loop(0, count, wrapped, 0)

    barrier = pltpu.get_barrier_semaphore()

    def greet(i):
        pz, pg = peer_at(i + 1)
        pl.semaphore_signal(barrier, inc=1, device_id=(pz, pg), device_id_type=mesh_type)

    loop(D - 1, greet)

    def enter(d):
        for k in range(K):
            at = pl.multiple_of(d * span + k * lanes, lanes)
            send[:, k, d] = spec_ref[:, :, pl.ds(at, lanes)]

    loop(D, enter)
    pl.semaphore_wait(barrier, D - 1)
    for chunk in range(chunks):
        start(0, chunk)

    rows_w = 16
    norm = 1.0 / math.sqrt(total)

    def prepare(b):
        k = lax.rem(b, K)
        r0 = pl.multiple_of(b // K * rows_w, rows_w)
        row = r0 + lax.broadcasted_iota(jnp.int32, (rows_w, lanes), 0)
        lane = lax.broadcasted_iota(jnp.int32, (rows_w, lanes), 1)
        col = me * span + k * lanes + lane
        angle = (row * col).astype(jnp.float32) * (2.0 * math.pi / total)
        t1[0, k, pl.ds(r0, rows_w)] = norm * jnp.cos(angle)
        t1[1, k, pl.ds(r0, rows_w)] = norm * jnp.sin(angle)
        for n, w in enumerate(weights_at(row * cols + col, total, par_ref[0])):
            wts[n, 0, k, pl.ds(r0, rows_w)] = w[0]
            wts[n, 1, k, pl.ds(r0, rows_w)] = w[1]

    loop(R // rows_w * K, prepare)

    def flat(ref):
        return ref.reshape(2, K, R, lanes)

    rb = min(128, R)

    def pair(ref, k, at):
        return ref[0, k, pl.ds(at, rb)], ref[1, k, pl.ds(at, rb)]

    def put(ref, k, at, value):
        ref[0, k, pl.ds(at, rb)] = value[0]
        ref[1, k, pl.ds(at, rb)] = value[1]

    def put_split(high, low, k, at, value):
        for part in range(2):
            h, l = split(value[part])
            k0 = k % part_k * lanes
            high[pl.ds(part * R + at, rb), k0 : k0 + lanes] = h
            low[pl.ds(part * R + at, rb), k0 : k0 + lanes] = l

    def column_dot(high, low, at):
        right = (high[...], low[...])
        return tuple(
            dot3((m1h[pl.ds(part * R + at, rb), :], m1l[pl.ds(part * R + at, rb), :]), right)
            for part in range(2)
        )

    def lane_block(value, k):
        k0 = k % part_k * lanes
        return value[:, k0 : k0 + lanes]

    def blocks(chunk):
        return range(chunk * part_k, (chunk + 1) * part_k)

    def row_at(b):
        return pl.multiple_of(b * rb, rb)

    send_flat = flat(send)

    def launch(slot, chunk):
        def body(b):
            at = row_at(b)
            real, imag = column_dot(xbh, xbl, at)
            for k in blocks(chunk):
                turned = times((lane_block(real, k), lane_block(imag, k)), pair(t1, k, at))
                put(send_flat, k, at, turned)

        loop(R // rb, body)
        start(slot, chunk)

    def land(slot, chunk, use):
        arrived = flat(recv.at[slot])

        def turn(b):
            at = row_at(b)
            for k in blocks(chunk):
                x = pair(arrived, k, at)
                t = pair(t1, k, at)
                value = (x[0] * t[0] + x[1] * t[1], x[0] * t[1] - x[1] * t[0])
                put_split(xah, xal, k, at, value)

        loop(R // rb, turn)

        def body(b):
            at = row_at(b)
            real, imag = column_dot(xah, xal, at)
            for k in blocks(chunk):
                use(k, at, (lane_block(real, k), -lane_block(imag, k)))

        loop(R // rb, body)

    group = 4
    lines_out = send.reshape(2 * A * sublanes, lanes)

    def physics(slot):
        lines_in = recv.at[slot].reshape(2 * A * sublanes, lanes)
        tr, ti = t2_ref[0], t2_ref[1]
        for base in range(0, sublanes, group):
            x = jnp.concatenate(
                [lines_in[pl.ds(base + g, 2 * A, stride=sublanes), :] for g in range(group)], axis=1
            )
            y = dot3((m2h[...], m2l[...]), split(x))
            parts = []
            for g in range(group):
                yr = y[:A, g * lanes : (g + 1) * lanes]
                yi = y[A:, g * lanes : (g + 1) * lanes]
                parts.append(jnp.concatenate([yr * tr - yi * ti, yr * ti + yi * tr], axis=1))
            u = dot3(split(jnp.concatenate(parts, axis=0)), (m3h[...], m3l[...]))
            ur, ui = u[:, :lanes], u[:, lanes:]
            mag = -(ur * ur + ui * ui)
            cubic = jnp.concatenate([mag * (ur - beta * ui), mag * (ui + beta * ur)], axis=1)
            y = dot3(split(cubic), (n3h[...], n3l[...]))
            parts = []
            for g in range(group):
                yr = y[g * A : (g + 1) * A, :lanes]
                yi = y[g * A : (g + 1) * A, lanes:]
                parts.append(jnp.concatenate([yr * tr + yi * ti, yi * tr - yr * ti], axis=0))
            h, l = split(jnp.concatenate(parts, axis=1))
            pxh[:, base * lanes : (base + group) * lanes] = h
            pxl[:, base * lanes : (base + group) * lanes] = l
        count = part_k * D
        for chunk in range(chunks):
            rows = pl.ds(chunk * 2 * count, 2 * count)
            x = dot3((n2h[rows, :], n2l[rows, :]), (pxh[...], pxl[...]))
            for part in range(2):
                for g in range(sublanes):
                    at = (part * K + chunk * part_k) * D * sublanes + g
                    lines_out[pl.ds(at, count, stride=sublanes), :] = x[
                        part * count : (part + 1) * count, g * lanes : (g + 1) * lanes
                    ]
            start(0, chunk)

    E, E2, Q, F1, F2, F3 = range(6)

    def weight(n, k, at):
        return pair(wts.at[n], k, at)

    def add(a, b):
        return a[0] + b[0], a[1] + b[1]

    first = flat(recv.at[0])
    for chunk in range(chunks):
        finish(0, chunk)

        def take(b):
            at = row_at(b)
            for k in blocks(chunk):
                v = pair(first, k, at)
                put_split(xbh, xbl, k, at, v)
                put(astate, k, at, v)

        loop(R // rb, take)
        launch(1, chunk)

    def hidden(body):
        def block(b):
            for k in range(K):
                body(k, row_at(b))

        loop(R // rb, block)

    def hide_start(k, at):
        v = pair(astate, k, at)
        put(acc, k, at, times(weight(E, k, at), v))
        put(pre, k, at, times(weight(E2, k, at), v))

    def use_first(k, at, n):
        a = add(pair(pre, k, at), times(weight(Q, k, at), n))
        put(nl, k, at, n)
        put(astate, k, at, a)
        put_split(xbh, xbl, k, at, a)

    def hide_first(k, at):
        n = pair(nl, k, at)
        put(acc, k, at, add(pair(acc, k, at), times(weight(F1, k, at), n)))
        qn = times(weight(Q, k, at), n)
        ea = times(weight(E2, k, at), pair(astate, k, at))
        put(astate, k, at, (ea[0] - qn[0], ea[1] - qn[1]))

    def use_second(k, at, n):
        b = add(pair(pre, k, at), times(weight(Q, k, at), n))
        put(nl, k, at, n)
        put_split(xbh, xbl, k, at, b)

    def hide_middle(k, at):
        n = pair(nl, k, at)
        put(acc, k, at, add(pair(acc, k, at), times(weight(F2, k, at), n)))

    def use_third(k, at, n):
        qn = times(weight(Q, k, at), n)
        put(nl, k, at, n)
        a = pair(astate, k, at)
        put_split(xbh, xbl, k, at, (a[0] + 2.0 * qn[0], a[1] + 2.0 * qn[1]))

    def use_last(k, at, n):
        put(send_flat, k, at, add(pair(acc, k, at), times(weight(F3, k, at), n)))

    uses = (use_first, use_second, use_third, use_last)
    hides = (hide_start, hide_first, hide_middle, hide_middle)
    for stage in range(4):
        hidden(hides[stage])
        for chunk in range(chunks):
            finish(1, chunk)
        physics(1)
        for chunk in range(chunks):
            finish(0, chunk)
            land(0, chunk, uses[stage])
            if stage < 3:
                launch(1, chunk)
            else:
                start(1, chunk)

    for chunk in range(chunks):
        finish(1, chunk)

        def leave(d):
            for k in blocks(chunk):
                at = pl.multiple_of(d * span + k * lanes, lanes)
                out_ref[:, :, pl.ds(at, lanes)] = recv[1, :, k, d]

        loop(D, leave)


def solution(mesh):
    axes = ("gx", "gy")
    Z, G = mesh.shape["gx"], mesh.shape["gy"]
    D = Z * G

    def local(spectrum, parameters):
        _, row_shard, columns = spectrum.shape
        assert row_shard == sublanes
        R = row_shard * D
        A = columns // lanes
        K = A // D
        assert K * D * lanes == columns
        counter = np.arange(R)
        m1 = halves(real_form(unit_roots(counter, counter, R)))
        order = (np.arange(D)[None, :] * K + np.arange(K)[:, None]).reshape(-1)
        m2_full = real_form(unit_roots(np.arange(A), order, A))
        chunks = 2 if K % 2 == 0 else 1
        sent = np.arange(2 * A).reshape(2, chunks, A // chunks).swapaxes(0, 1).reshape(-1)
        m2, n2 = halves(m2_full), halves(m2_full.T[sent])
        m3_full = real_form(unit_roots(np.arange(lanes), np.arange(lanes), lanes)).T
        m3, n3 = halves(m3_full), halves(m3_full.T)
        turn = unit_roots(np.arange(A), np.arange(lanes), columns)
        t2 = jnp.asarray(np.stack([turn.real, turn.imag]), jnp.float32)
        vmem = pl.BlockSpec(memory_space=pltpu.VMEM)
        state = pltpu.VMEM((2, K, R, lanes), jnp.float32)
        half = pltpu.VMEM((2 * R, K // chunks * lanes), jnp.bfloat16)
        line = pltpu.VMEM((2 * A, sublanes * lanes), jnp.bfloat16)
        return pl.pallas_call(
            functools.partial(kernel, axes, (Z, G, D, K, R)),
            out_shape=jax.ShapeDtypeStruct(spectrum.shape, jnp.float32),
            in_specs=[pl.BlockSpec(memory_space=pltpu.SMEM)] + [vmem] * 12,
            out_specs=vmem,
            scratch_shapes=[
                pltpu.VMEM((2, K, D, sublanes, lanes), jnp.float32),
                pltpu.VMEM((2, 2, K, D, sublanes, lanes), jnp.float32),
                pltpu.VMEM((6, 2, K, R, lanes), jnp.float32),
                state, state, state, state, state,
                half, half, half, half, line, line,
                pltpu.SemaphoreType.DMA((chunks, D)),
                pltpu.SemaphoreType.DMA((2, chunks, D)),
            ],
            compiler_params=pltpu.CompilerParams(
                collective_id=0, has_side_effects=True, vmem_limit_bytes=60 * 1024 * 1024
            ),
        )(parameters, spectrum, *m1, *m2, *n2, *m3, *n3, t2)

    return jax.shard_map(
        local,
        mesh=mesh,
        in_specs=(P(None, axes, None), P()),
        out_specs=P(None, axes, None),
        check_vma=False,
    )
```

```python
import functools
import math

import jax
import jax.numpy as jnp
import numpy as np
from jax import lax
from jax.experimental import pallas as pl
from jax.experimental.pallas import tpu as pltpu
from jax.sharding import PartitionSpec as P

time_step = 0.1
spacing = 0.25
lanes = 128
sublanes = 8


def real_form(matrix):
    return np.block([[matrix.real, -matrix.imag], [matrix.imag, matrix.real]])


def halves(matrix):
    high = jnp.asarray(matrix, jnp.float32).astype(jnp.bfloat16)
    low = (jnp.asarray(matrix, jnp.float32) - high.astype(jnp.float32)).astype(jnp.bfloat16)
    return high, low


def unit_roots(left, right, length):
    product = (left[:, None].astype(np.int64) * right[None, :].astype(np.int64)) % length
    return np.exp(2j * np.pi * product / length)


def split(value):
    high = value.astype(jnp.bfloat16)
    return high, (value - high.astype(jnp.float32)).astype(jnp.bfloat16)


def dot(a, b):
    return jnp.dot(a, b, preferred_element_type=jnp.float32)


def dot3(left, right):
    return dot(left[0], right[0]) + dot(left[0], right[1]) + dot(left[1], right[0])


def times(a, b):
    return a[0] * b[0] - a[1] * b[1], a[0] * b[1] + a[1] * b[0]


def phi_values(w, orders):
    inside = w[0] * w[0] + w[1] * w[1] < 1.0
    g = (jnp.where(inside, 1.0, w[0]), jnp.where(inside, 0.0, w[1]))
    inverse = 1.0 / (g[0] * g[0] + g[1] * g[1])
    inv = (g[0] * inverse, -g[1] * inverse)
    growth = jnp.exp(g[0])
    direct = []
    last = (growth * jnp.cos(g[1]), growth * jnp.sin(g[1]))
    for k in range(orders):
        last = times((last[0] - 1.0 / math.factorial(k), last[1]), inv)
        direct.append(last)
    running = (
        jnp.full_like(w[0], 1.0 / math.factorial(14 + orders)),
        jnp.zeros_like(w[0]),
    )
    for degree in range(13, -1, -1):
        running = times(running, w)
        running = (running[0] + 1.0 / math.factorial(degree + orders), running[1])
    series = [running]
    for k in range(orders - 1, 0, -1):
        running = times(running, w)
        running = (running[0] + 1.0 / math.factorial(k), running[1])
        series.insert(0, running)
    return [
        (jnp.where(inside, s[0], d[0]), jnp.where(inside, s[1], d[1]))
        for s, d in zip(series, direct)
    ]


def weights_at(mode, modes_total, dispersion):
    signed = jnp.where(mode < modes_total // 2, mode, mode - modes_total).astype(jnp.float32)
    wavenum = signed * (2.0 * math.pi / (modes_total * spacing))
    square = wavenum * wavenum
    zeta = (time_step * (1.0 - square), -(time_step * dispersion * square))
    half = (0.5 * zeta[0], 0.5 * zeta[1])
    one, two, three = phi_values(zeta, 3)
    (half_one,) = phi_values(half, 1)
    grow = jnp.exp(half[0])
    e2 = (grow * jnp.cos(half[1]), grow * jnp.sin(half[1]))
    full = times(e2, e2)
    h = time_step
    q = tuple(0.5 * h * x for x in half_one)
    f1 = tuple(h * (a - 3.0 * b + 4.0 * c) for a, b, c in zip(one, two, three))
    f2 = tuple(2.0 * h * (b - 2.0 * c) for b, c in zip(two, three))
    f3 = tuple(h * (4.0 * c - b) for b, c in zip(two, three))
    return full, e2, q, f1, f2, f3


def kernel(
    axes, sizes,
    par_ref, spec_ref, m1h, m1l, m2h, m2l, n2h, n2l, m3h, m3l, n3h, n3l, t2_ref,
    out_ref,
    send, recv, wts, t1, pre, acc, astate, nl, xah, xal, xbh, xbl, pxh, pxl, send_sem, recv_sem,
):
    Z, G, D, K, R = sizes
    A = K * D
    cols = A * lanes
    span = K * lanes
    total = R * cols
    zi = lax.axis_index(axes[0])
    gi = lax.axis_index(axes[1])
    me = zi * G + gi
    mesh_type = pl.DeviceIdType.MESH
    beta = par_ref[1]

    chunks = 2 if K % 2 == 0 else 1
    part_k = K // chunks

    def peer_at(i):
        mask = D - i
        if D & (D - 1) == 0:
            peer, bit = 0, 1
            while bit < D:
                peer = peer + lax.rem(me // bit + mask // bit, 2) * bit
                bit *= 2
        else:
            peer = lax.rem(me + mask, D)
        return peer // G, lax.rem(peer, G)

    def copy(slot, chunk, i, landing):
        pz, pg = peer_at(i)
        peer = pz * G + pg
        at = me if landing is None else peer
        ks = pl.ds(chunk * part_k, part_k)
        return pltpu.make_async_remote_copy(
            src_ref=send.at[:, ks, peer],
            dst_ref=recv.at[slot, :, ks, at],
            send_sem=send_sem.at[chunk, peer],
            recv_sem=recv_sem.at[slot, chunk, at],
            device_id=(pz, pg),
            device_id_type=mesh_type,
        )

    def blocks(chunk):
        return [(place, chunk * part_k + place) for place in range(part_k)]

    def start(slot, chunk):
        def body(i, carry):
            copy(slot, chunk, i, None).start()
            return carry

        lax.fori_loop(1, D, body, 0)
        for _, k in blocks(chunk):
            recv[slot, :, k, me] = send[:, k, me]

    def finish(slot, chunk):
        def body(i, carry):
            arriving = copy(slot, chunk, i, True)
            arriving.wait_recv()
            arriving.wait_send()
            return carry

        lax.fori_loop(1, D, body, 0)

    def loop(count, body):
        def wrapped(i, carry):
            body(i)
            return carry

        lax.fori_loop(0, count, wrapped, 0)

    barrier = pltpu.get_barrier_semaphore()

    def greet(i):
        pz, pg = peer_at(i + 1)
        pl.semaphore_signal(barrier, inc=1, device_id=(pz, pg), device_id_type=mesh_type)

    loop(D - 1, greet)

    def enter(d):
        for k in range(K):
            at = pl.multiple_of(d * span + k * lanes, lanes)
            send[:, k, d] = spec_ref[:, :, pl.ds(at, lanes)]

    loop(D, enter)
    pl.semaphore_wait(barrier, D - 1)
    for chunk in range(chunks):
        start(0, chunk)

    rows_w = 16
    norm = 1.0 / math.sqrt(total)

    def prepare(b):
        k = lax.rem(b, K)
        r0 = pl.multiple_of(b // K * rows_w, rows_w)
        row = r0 + lax.broadcasted_iota(jnp.int32, (rows_w, lanes), 0)
        lane = lax.broadcasted_iota(jnp.int32, (rows_w, lanes), 1)
        col = me * span + k * lanes + lane
        angle = (row * col).astype(jnp.float32) * (2.0 * math.pi / total)
        t1[0, k, pl.ds(r0, rows_w)] = norm * jnp.cos(angle)
        t1[1, k, pl.ds(r0, rows_w)] = norm * jnp.sin(angle)
        for n, w in enumerate(weights_at(row * cols + col, total, par_ref[0])):
            wts[n, 0, k, pl.ds(r0, rows_w)] = w[0]
            wts[n, 1, k, pl.ds(r0, rows_w)] = w[1]

    loop(R // rows_w * K, prepare)

    def flat(ref):
        return ref.reshape(2, K, R, lanes)

    rb = min(128, R)

    def pair(ref, k, at):
        return ref[0, k, pl.ds(at, rb)], ref[1, k, pl.ds(at, rb)]

    def put(ref, k, at, value):
        ref[0, k, pl.ds(at, rb)] = value[0]
        ref[1, k, pl.ds(at, rb)] = value[1]

    def put_split(high, low, place, at, value):
        for part in range(2):
            h, l = split(value[part])
            k0 = place * lanes
            high[pl.ds(part * R + at, rb), k0 : k0 + lanes] = h
            low[pl.ds(part * R + at, rb), k0 : k0 + lanes] = l

    def column_dot(high, low, at):
        right = (high[...], low[...])
        return tuple(
            dot3((m1h[pl.ds(part * R + at, rb), :], m1l[pl.ds(part * R + at, rb), :]), right)
            for part in range(2)
        )

    def lane_block(value, place):
        return value[:, place * lanes : (place + 1) * lanes]

    def row_at(b):
        return pl.multiple_of(b * rb, rb)

    send_flat = flat(send)

    def launch(slot, chunk):
        def body(b):
            at = row_at(b)
            real, imag = column_dot(xbh, xbl, at)
            for place, k in blocks(chunk):
                turned = times((lane_block(real, place), lane_block(imag, place)), pair(t1, k, at))
                put(send_flat, k, at, turned)

        loop(R // rb, body)
        start(slot, chunk)

    def land(slot, chunk, use):
        arrived = flat(recv.at[slot])

        def turn(b):
            at = row_at(b)
            for place, k in blocks(chunk):
                x = pair(arrived, k, at)
                t = pair(t1, k, at)
                value = (x[0] * t[0] + x[1] * t[1], x[0] * t[1] - x[1] * t[0])
                put_split(xah, xal, place, at, value)

        loop(R // rb, turn)

        def body(b):
            at = row_at(b)
            real, imag = column_dot(xah, xal, at)
            for place, k in blocks(chunk):
                use(place, k, at, (lane_block(real, place), -lane_block(imag, place)))

        loop(R // rb, body)

    group = 4
    lines_out = send.reshape(2 * A * sublanes, lanes)

    def physics(slot):
        lines_in = recv.at[slot].reshape(2 * A * sublanes, lanes)
        tr, ti = t2_ref[0], t2_ref[1]
        for base in range(0, sublanes, group):
            x = jnp.concatenate(
                [lines_in[pl.ds(base + g, 2 * A, stride=sublanes), :] for g in range(group)], axis=1
            )
            y = dot3((m2h[...], m2l[...]), split(x))
            parts = []
            for g in range(group):
                yr = y[:A, g * lanes : (g + 1) * lanes]
                yi = y[A:, g * lanes : (g + 1) * lanes]
                parts.append(jnp.concatenate([yr * tr - yi * ti, yr * ti + yi * tr], axis=1))
            u = dot3(split(jnp.concatenate(parts, axis=0)), (m3h[...], m3l[...]))
            ur, ui = u[:, :lanes], u[:, lanes:]
            mag = -(ur * ur + ui * ui)
            cubic = jnp.concatenate([mag * (ur - beta * ui), mag * (ui + beta * ur)], axis=1)
            y = dot3(split(cubic), (n3h[...], n3l[...]))
            parts = []
            for g in range(group):
                yr = y[g * A : (g + 1) * A, :lanes]
                yi = y[g * A : (g + 1) * A, lanes:]
                parts.append(jnp.concatenate([yr * tr + yi * ti, yi * tr - yr * ti], axis=0))
            h, l = split(jnp.concatenate(parts, axis=1))
            pxh[:, base * lanes : (base + group) * lanes] = h
            pxl[:, base * lanes : (base + group) * lanes] = l
        count = part_k * D
        for chunk in range(chunks):
            rows = pl.ds(chunk * 2 * count, 2 * count)
            x = dot3((n2h[rows, :], n2l[rows, :]), (pxh[...], pxl[...]))
            for part in range(2):
                for g in range(sublanes):
                    at = (part * K + chunk * part_k) * D * sublanes + g
                    lines_out[pl.ds(at, count, stride=sublanes), :] = x[
                        part * count : (part + 1) * count, g * lanes : (g + 1) * lanes
                    ]
            start(0, chunk)

    E, E2, Q, F1, F2, F3 = range(6)

    def weight(n, k, at):
        return pair(wts.at[n], k, at)

    def add(a, b):
        return a[0] + b[0], a[1] + b[1]

    first = flat(recv.at[0])
    for chunk in range(chunks):
        finish(0, chunk)

        def take(b):
            at = row_at(b)
            for place, k in blocks(chunk):
                v = pair(first, k, at)
                put_split(xbh, xbl, place, at, v)
                put(astate, k, at, v)

        loop(R // rb, take)
        launch(1, chunk)

    def hidden(body):
        def block(b):
            body(lax.rem(b, K), row_at(b // K))

        loop(R // rb * K, block)

    def hide_start(k, at):
        v = pair(astate, k, at)
        put(acc, k, at, times(weight(E, k, at), v))
        put(pre, k, at, times(weight(E2, k, at), v))

    def use_first(place, k, at, n):
        a = add(pair(pre, k, at), times(weight(Q, k, at), n))
        put(nl, k, at, n)
        put(astate, k, at, a)
        put_split(xbh, xbl, place, at, a)

    def hide_first(k, at):
        n = pair(nl, k, at)
        put(acc, k, at, add(pair(acc, k, at), times(weight(F1, k, at), n)))
        qn = times(weight(Q, k, at), n)
        ea = times(weight(E2, k, at), pair(astate, k, at))
        put(astate, k, at, (ea[0] - qn[0], ea[1] - qn[1]))

    def use_second(place, k, at, n):
        b = add(pair(pre, k, at), times(weight(Q, k, at), n))
        put(nl, k, at, n)
        put_split(xbh, xbl, place, at, b)

    def hide_middle(k, at):
        n = pair(nl, k, at)
        put(acc, k, at, add(pair(acc, k, at), times(weight(F2, k, at), n)))

    def use_third(place, k, at, n):
        qn = times(weight(Q, k, at), n)
        put(nl, k, at, n)
        a = pair(astate, k, at)
        put_split(xbh, xbl, place, at, (a[0] + 2.0 * qn[0], a[1] + 2.0 * qn[1]))

    def use_last(place, k, at, n):
        put(send_flat, k, at, add(pair(acc, k, at), times(weight(F3, k, at), n)))

    uses = (use_first, use_second, use_third, use_last)
    hides = (hide_start, hide_first, hide_middle, hide_middle)
    for stage in range(4):
        hidden(hides[stage])
        for chunk in range(chunks):
            finish(1, chunk)
        physics(1)

        def column_side(chunk):
            finish(0, chunk)
            land(0, chunk, uses[stage])
            if stage < 3:
                launch(1, chunk)
            else:
                start(1, chunk)

        loop(chunks, column_side)

    for chunk in range(chunks):
        finish(1, chunk)

        def leave(d):
            for place, k in blocks(chunk):
                at = pl.multiple_of(d * span + k * lanes, lanes)
                out_ref[:, :, pl.ds(at, lanes)] = recv[1, :, k, d]

        loop(D, leave)


def solution(mesh):
    axes = ("gx", "gy")
    Z, G = mesh.shape["gx"], mesh.shape["gy"]
    D = Z * G

    def local(spectrum, parameters):
        _, row_shard, columns = spectrum.shape
        assert row_shard == sublanes
        R = row_shard * D
        A = columns // lanes
        K = A // D
        assert K * D * lanes == columns
        counter = np.arange(R)
        m1 = halves(real_form(unit_roots(counter, counter, R)))
        order = (np.arange(D)[None, :] * K + np.arange(K)[:, None]).reshape(-1)
        m2_full = real_form(unit_roots(np.arange(A), order, A))
        chunks = 2 if K % 2 == 0 else 1
        sent = np.arange(2 * A).reshape(2, chunks, A // chunks).swapaxes(0, 1).reshape(-1)
        m2, n2 = halves(m2_full), halves(m2_full.T[sent])
        m3_full = real_form(unit_roots(np.arange(lanes), np.arange(lanes), lanes)).T
        m3, n3 = halves(m3_full), halves(m3_full.T)
        turn = unit_roots(np.arange(A), np.arange(lanes), columns)
        t2 = jnp.asarray(np.stack([turn.real, turn.imag]), jnp.float32)
        vmem = pl.BlockSpec(memory_space=pltpu.VMEM)
        state = pltpu.VMEM((2, K, R, lanes), jnp.float32)
        half = pltpu.VMEM((2 * R, K // chunks * lanes), jnp.bfloat16)
        line = pltpu.VMEM((2 * A, sublanes * lanes), jnp.bfloat16)
        return pl.pallas_call(
            functools.partial(kernel, axes, (Z, G, D, K, R)),
            out_shape=jax.ShapeDtypeStruct(spectrum.shape, jnp.float32),
            in_specs=[pl.BlockSpec(memory_space=pltpu.SMEM)] + [vmem] * 12,
            out_specs=vmem,
            scratch_shapes=[
                pltpu.VMEM((2, K, D, sublanes, lanes), jnp.float32),
                pltpu.VMEM((2, 2, K, D, sublanes, lanes), jnp.float32),
                pltpu.VMEM((6, 2, K, R, lanes), jnp.float32),
                state, state, state, state, state,
                half, half, half, half, line, line,
                pltpu.SemaphoreType.DMA((chunks, D)),
                pltpu.SemaphoreType.DMA((2, chunks, D)),
            ],
            compiler_params=pltpu.CompilerParams(
                collective_id=0, has_side_effects=True, vmem_limit_bytes=60 * 1024 * 1024
            ),
        )(parameters, spectrum, *m1, *m2, *n2, *m3, *n3, t2)

    return jax.shard_map(
        local,
        mesh=mesh,
        in_specs=(P(None, axes, None), P()),
        out_specs=P(None, axes, None),
        check_vma=False,
    )
```
